256 devices in a mesh: latent: 64 (over y, x_hi, z), dp: 4 (over x_lo, core).
Axes of the slice: x: 4 (x_hi: 2, x_lo: 2; x = x_hi * 2 + x_lo), y: 4, z: 8, core: 2. Of those that a mesh axis runs over, the one named last changes fastest.
Arguments:
- codes_val: bfloat16 [256, 64], replicated, may hold values from 0.049804688 to 4
- codes_idx: int32 [256, 64], replicated, may hold values from 0 to 98303, as said below
- target: bfloat16 [256, 6144], P(('latent', 'dp')), may hold values from -6 to 6
- dec_weight: bfloat16 [98304, 6144], P(('latent', 'dp')), may hold values from -0.75 to 0.75
- dec_bias: float32 [6144], replicated, may hold values from -3 to 3
- basis: float32 [6144, 256], P('dp'), may hold values from -0.375 to 0.375
- first_mom: float32 [98304, 256], P(('latent', 'dp')), may hold values from -3 to 3
- second_mom: float32 [98304, 256], P(('latent', 'dp')), may hold values from 0.02 to 0.2
Outputs:
- update: bfloat16 [98304, 6144], P(('latent', 'dp'))
- first_new: float32 [98304, 256], P(('latent', 'dp'))
- second_new: float32 [98304, 256], P(('latent', 'dp'))
- code_grad: float32 [256, 64], P(('latent', 'dp'))
The draws below stay inside these ranges and needn't reach their ends.
Inputs may be any that keep to these rules, and one draw needn't show every extreme that they name: `codes_idx`: A token's 64 latent numbers are distinct. Number the devices in the order latent then dp; device s holds latents s * 384 to (s + 1) * 384 - 1 and the token rows of its block of 256 / (64 * 4). Of the active pairs of one device's token rows, at most 1 fall in one device's latents, and in every such block some device's latents receive exactly 1.
All inputs are finite; a program needn't handle non-finite values.
Results may differ from the reference program's by a relative error of at most 0.0038.
Values may be sent and summed in bfloat16 or wider, within the bound.
No kernel may reach another device: no remote copies, remote signals or barrier semaphores. Data moves between devices by JAX's collectives and lax.ppermute only.
A program may use at most 128 MiB of HBM per device.

```python
import math
import jax
import jax.numpy as jnp
from jax import lax

D = 6144
LAT_DEV = 384
TOPK = 64
RANK = 256
TOKENS = 256
LATENTS = 98304
CAP = 1
DEVICES = 256


def draw_codes_idx(key, part):
    pairs = TOKENS * TOPK // DEVICES
    total = CAP * DEVICES

    def one_block(block_key):
        key_perm, key_mix, key_shift, key_base = jax.random.split(block_key, 4)
        order_one = jax.random.permutation(key_perm, total).astype(jnp.int32)
        owner_slab = order_one % DEVICES
        leader = owner_slab[0]
        ranking = jnp.where(owner_slab == leader, 0, 1).astype(jnp.int32) * total + jnp.arange(total, dtype=jnp.int32)
        chosen = order_one[jnp.argsort(ranking)][:pairs]
        mixed = jax.random.permutation(key_mix, chosen).astype(jnp.int32)
        slab = mixed % DEVICES
        within = mixed // DEVICES
        shifts = jax.random.randint(key_shift, (DEVICES,), 0, CAP).astype(jnp.int32)
        base = jax.random.randint(key_base, (pairs,), 0, LAT_DEV // CAP).astype(jnp.int32)
        offset = base * CAP + (within + shifts[slab]) % CAP
        return slab * LAT_DEV + offset
    keys = jax.random.split(jax.random.fold_in(key, 7), DEVICES)
    return jax.vmap(one_block)(keys).reshape(TOKENS, TOPK).astype(jnp.int32)


def block_scale(stream_key, shape, pieces, least, top_value):
    gain = 1.0
    for dim, shards_of in pieces:
        steps = jax.random.uniform(jax.random.fold_in(jax.random.fold_in(stream_key, 6), dim), (shards_of,), jnp.float32, least / len(pieces), top_value / len(pieces))
        gain = gain * jnp.repeat(jnp.exp(steps), shape[dim] // shards_of).reshape((-1,) + (1,) * (len(shape) - 1 - dim))
    return gain


def gaussian(key, shape, scale, limit, shards=(), held_as=jnp.bfloat16):
    factor_of = block_scale(key, shape, shards, -0.22, 0.18) if shards else 1.0
    array = jax.random.normal(key, shape, jnp.float32) * scale * factor_of
    return jnp.minimum(jnp.maximum(array, -limit), limit).astype(held_as)


def setup_inputs(seed: int = 0) -> dict:
    streams_of = jax.random.split(jax.random.key(seed), 9)
    return {
        "codes_val": jnp.clip(jnp.exp(jax.random.uniform(streams_of[0], (TOKENS, TOPK), jnp.float32, math.log(0.049804688), math.log(4.0))), 0.049804688, 4.0).astype(jnp.bfloat16),
        "codes_idx": draw_codes_idx(jax.random.fold_in(streams_of[8], 71), 0),
        "target": gaussian(streams_of[2], (TOKENS, D), 1.0, 6.0, ((0, 256),)),
        "dec_weight": gaussian(streams_of[3], (LATENTS, D), TOPK ** -0.5, 0.75, ((0, 256),)),
        "dec_bias": gaussian(streams_of[4], (D,), 0.5, 3.0, (), jnp.float32),
        "basis": gaussian(streams_of[5], (D, RANK), RANK ** -0.5, 0.375, ((0, 4),), jnp.float32),
        "first_mom": gaussian(streams_of[6], (LATENTS, RANK), 0.5, 3.0, ((0, 256),), jnp.float32),
        "second_mom": jnp.clip(jnp.exp(math.log(0.2) - 2.3025851 * jax.random.uniform(streams_of[7], (LATENTS, RANK), jnp.float32) ** block_scale(streams_of[7], (LATENTS, RANK), ((0, 256),), -0.2, 0.2)), 0.02, 0.2),
    }


beta_one = 0.9
beta_two = 0.999
epsilon = 1e-08
first_fix = 1.0 - math.exp(100.0 * math.log(0.9))
second_fix = 1.0 - math.exp(100.0 * math.log(0.999))

def row_step(rows):
    return 64 if rows % 64 == 0 else rows

def spread_codes(values, indices, start, width):
    local = indices - start
    inside = (local >= 0) & (local < width)
    slot = jnp.where(inside, local, width).astype(jnp.int32)
    rows = indices.shape[0]
    topk = indices.shape[1]
    step = row_step(rows)
    columns = jnp.arange(width, dtype=jnp.int32)

    def one_block(pair):
        block_val, block_slot = pair
        hit = block_slot[:, :, None] == columns[None, None, :]
        return lax.optimization_barrier(jnp.sum(jnp.where(hit, block_val.astype(jnp.float32)[:, :, None], jnp.float32(0.0)), axis=1))
    dense = lax.map(one_block, (values.reshape(rows // step, step, topk), slot.reshape(rows // step, step, topk)))
    dense = dense.reshape(rows, width)
    return (dense.astype(jnp.bfloat16), inside, jnp.where(inside, local, 0).astype(jnp.int32))

def pick_columns(matrix, slot):
    rows = slot.shape[0]
    topk = slot.shape[1]
    width = matrix.shape[1]
    step = row_step(rows)
    columns = jnp.arange(width, dtype=jnp.int32)

    def one_block(pair):
        block_mat, block_slot = pair
        hit = block_slot[:, :, None] == columns[None, None, :]
        return lax.optimization_barrier(jnp.sum(jnp.where(hit, block_mat[:, None, :], jnp.float32(0.0)), axis=2))
    picked = lax.map(one_block, (matrix.reshape(rows // step, step, width), slot.reshape(rows // step, step, topk)))
    return picked.reshape(rows, topk)

def reference(codes_val, codes_idx, target, dec_weight, dec_bias, basis, first_mom, second_mom):
    blocks = LATENTS // LAT_DEV
    numbers = jnp.arange(blocks, dtype=jnp.int32)

    def forward(total, block):
        start = (block * LAT_DEV).astype(jnp.int32)
        codes, inside, slot = spread_codes(codes_val, codes_idx, start, LAT_DEV)
        weight = lax.dynamic_slice_in_dim(dec_weight, start, LAT_DEV, 0)
        return (total + jnp.dot(codes, weight, preferred_element_type=jnp.float32), None)
    recon, unused = lax.scan(forward, jnp.zeros((TOKENS, D), jnp.float32), numbers)
    resid = (recon + dec_bias - target.astype(jnp.float32)).astype(jnp.bfloat16)

    def backward(carried, block):
        start = (block * LAT_DEV).astype(jnp.int32)
        codes, inside, slot = spread_codes(codes_val, codes_idx, start, LAT_DEV)
        weight = lax.dynamic_slice_in_dim(dec_weight, start, LAT_DEV, 0)
        grad = jnp.dot(codes.T, resid, preferred_element_type=jnp.float32)
        proj = jnp.dot(grad, basis, precision=lax.Precision.HIGHEST, preferred_element_type=jnp.float32)
        first = lax.dynamic_slice_in_dim(first_mom, start, LAT_DEV, 0)
        second = lax.dynamic_slice_in_dim(second_mom, start, LAT_DEV, 0)
        first_out = beta_one * first + (1.0 - beta_one) * proj
        second_out = beta_two * second + (1.0 - beta_two) * proj * proj
        normed = first_out / first_fix / (jnp.sqrt(second_out / second_fix) + epsilon)
        update = jnp.dot(normed, basis.T, precision=lax.Precision.HIGHEST, preferred_element_type=jnp.float32).astype(jnp.bfloat16)
        back = jnp.dot(resid, weight.T, preferred_element_type=jnp.float32)
        picked = jnp.where(inside, pick_columns(back, slot), 0.0)
        return (carried + picked, (update, first_out, second_out))
    code_grad, outputs = lax.scan(backward, jnp.zeros((TOKENS, TOPK), jnp.float32), numbers)
    update, first_out, second_out = outputs
    return (update.reshape(LATENTS, D), first_out.reshape(LATENTS, RANK), second_out.reshape(LATENTS, RANK), code_grad)
```

```python
import math

import jax
import jax.numpy as jnp
from jax import lax
from jax.experimental import pallas as pl
from jax.experimental.pallas import tpu as pltpu
from jax.sharding import Mesh
from jax.sharding import PartitionSpec as P

AXES = ("y", "x_hi", "z", "x_lo", "core")
PLANE = ("y", "x_hi", "x_lo", "core")
RING = ("x_hi", "x_lo", "core")

beta_one = 0.9
beta_two = 0.999
epsilon = 1e-08
first_fix = 1.0 - math.exp(100.0 * math.log(0.9))
second_fix = 1.0 - math.exp(100.0 * math.log(0.999))

LAT = 384
TOK = 256
TOPK = 64
MODEL = 6144
RANK = 256
PIECE = MODEL // 4
BF = jnp.bfloat16
F32 = jnp.float32
VMEM = pltpu.VMEM


def iota(shape, dim):
    return lax.broadcasted_iota(jnp.int32, shape, dim)


def dot_nt(a, b):
    return lax.dot_general(a, b, (((1,), (1,)), ((), ())), preferred_element_type=F32)


def slab_of(idx):
    return jnp.floor((idx.astype(F32) + 0.5) * (1.0 / LAT))


def pack_kernel(place, idx_ref, val_ref, weight_ref, sent_ref, codes_ref, hot_ref):
    @pl.when(pl.program_id(0) == 0)
    def _():
        me = place[0]
        idx = idx_ref[...]
        inside = slab_of(idx) == me.astype(F32)
        local = jnp.sum(jnp.where(inside, idx - me * LAT + 1, 0), axis=0, keepdims=True) - 1
        value = jnp.sum(
            jnp.where(inside, val_ref[...].astype(F32), 0.0), axis=0, keepdims=True
        )
        hit = iota((LAT, TOK), 0) == local
        row = iota((TOK, TOK), 0)
        token = (row >> 5) * 32 + (row & 7) * 4 + ((row >> 3) & 3)
        order = jnp.where(iota((TOK, TOK), 1) == token, 1.0, 0.0).astype(BF)
        hot_ref[...] = dot_nt(order, jnp.where(hit, 1.0, 0.0).astype(BF)).astype(BF)
        codes_ref[...] = dot_nt(jnp.where(hit, value, 0.0).astype(BF), order).astype(BF)

    sent_ref[...] = jnp.dot(
        hot_ref[...], weight_ref[...], preferred_element_type=F32
    ).astype(BF)


def pack(place, idx_t, val_t, weight):
    step = 768
    return pl.pallas_call(
        pack_kernel,
        grid_spec=pltpu.PrefetchScalarGridSpec(
            num_scalar_prefetch=1,
            grid=(MODEL // step,),
            in_specs=[
                pl.BlockSpec((TOPK, TOK), lambda j, s: (0, 0)),
                pl.BlockSpec((TOPK, TOK), lambda j, s: (0, 0)),
                pl.BlockSpec((LAT, step), lambda j, s: (0, j)),
            ],
            out_specs=[
                pl.BlockSpec((TOK, step), lambda j, s: (0, j)),
                pl.BlockSpec((LAT, TOK), lambda j, s: (0, 0)),
            ],
            scratch_shapes=[pltpu.VMEM((TOK, LAT), BF)],
        ),
        out_shape=[
            jax.ShapeDtypeStruct((TOK, MODEL), BF),
            jax.ShapeDtypeStruct((LAT, TOK), BF),
        ],
        cost_estimate=pl.CostEstimate(
            flops=2 * TOK * LAT * MODEL, bytes_accessed=8_000_000, transcendentals=0
        ),
        name="pack",
    )(place, idx_t, val_t, weight)


def recon_kernel(place, idx_ref, val_ref, recv_ref, part_ref, slab_ref):
    z = place[3]
    token = place[1] * 32 + iota((8, TOK), 0) * 4 + place[2]
    pick = jnp.where(iota((8, TOK), 1) == token, 1.0, 0.0).astype(BF)
    slab = dot_nt(pick, slab_of(idx_ref[...]).astype(BF))
    value = dot_nt(pick, val_ref[...])
    slab_ref[...] = slab
    lane = iota((8, TOK), 1)
    source = ((lane >> 5) * 32 + ((lane >> 3) & 3) + z * 4).astype(F32)
    weight = jnp.zeros((8, TOK), F32)
    for k in range(TOPK):
        weight += jnp.where(slab[:, k : k + 1] == source, value[:, k : k + 1], 0.0)
    weight = jnp.where((lane & 7) == iota((8, TOK), 0), weight, 0.0).astype(BF)
    step = 1024
    for j in range(MODEL // step):
        part_ref[:, j * step : (j + 1) * step] = jnp.dot(
            weight, recv_ref[:, j * step : (j + 1) * step], preferred_element_type=F32
        )


def whole(n):
    return [pl.BlockSpec(memory_space=pltpu.VMEM)] * n


SMEM = pl.BlockSpec(memory_space=pltpu.SMEM)


def partial_recon(place, idx_t, val_t, recv):
    return pl.pallas_call(
        recon_kernel,
        in_specs=[SMEM] + whole(3),
        out_specs=whole(2),
        out_shape=[
            jax.ShapeDtypeStruct((8, MODEL), F32),
            jax.ShapeDtypeStruct((8, TOPK), F32),
        ],
        cost_estimate=pl.CostEstimate(
            flops=2 * TOK * 8 * MODEL, bytes_accessed=4_000_000, transcendentals=0
        ),
        name="partial_recon",
    )(place, idx_t, val_t, recv)


def back_kernel(place, resid_ref, recv_ref, slab_ref, b0, b1, b2, b3, cg_ref, proj_ref):
    z = place[3]
    block = place[4]
    proj = jnp.zeros((8, RANK), F32)
    for g, ref in enumerate((b0, b1, b2, b3)):
        at = pl.multiple_of((block ^ g) * PIECE, 128)
        proj += jnp.dot(resid_ref[:, pl.ds(at, PIECE)], ref[...], preferred_element_type=F32)
    proj_ref[...] = jnp.broadcast_to(proj[None], (32, 8, RANK))
    dots = dot_nt(resid_ref[...], recv_ref[...])
    lane = iota((8, TOK), 1)
    dots = jnp.where((lane & 7) == iota((8, TOK), 0), dots, 0.0)
    member = jnp.where(iota((TOK, 128), 0) >> 3 == iota((TOK, 128), 1), 1.0, 0.0)
    dots = jnp.dot(
        dots, member, precision=lax.Precision.HIGHEST, preferred_element_type=F32
    )
    slab = slab_ref[...]
    grad = jnp.zeros((8, TOPK), F32)
    for p in range(32):
        source = ((p >> 2) * 32 + (p & 3) + z * 4).astype(F32)
        grad += jnp.where(slab == source, dots[:, p : p + 1], 0.0)
    cg_ref[:, 0:TOPK] = grad
    cg_ref[:, TOPK:] = jnp.zeros((8, 128 - TOPK), F32)


def back(place, resid, recv, slab, pieces):
    return pl.pallas_call(
        back_kernel,
        in_specs=[SMEM] + whole(7),
        out_specs=whole(2),
        out_shape=[
            jax.ShapeDtypeStruct((8, 128), F32),
            jax.ShapeDtypeStruct((32, 8, RANK), F32),
        ],
        cost_estimate=pl.CostEstimate(
            flops=2 * TOK * 8 * MODEL * 2, bytes_accessed=7_000_000, transcendentals=0
        ),
        name="back",
    )(place, resid, recv, slab, *pieces)


def update_kernel(
    place, codes_ref, proj_ref, first_ref, second_ref, b0, b1, b2, b3,
    out_ref, first_out_ref, second_out_ref, high_ref, low_ref,
):
    g = pl.program_id(0)
    j = pl.program_id(1)

    @pl.when((g == 0) & (j == 0))
    def _():
        proj_tok = proj_ref[...]
        codes = codes_ref[...]
        one = proj_tok.astype(BF)
        rest = proj_tok - one.astype(F32)
        two = rest.astype(BF)
        three = (rest - two.astype(F32)).astype(BF)
        proj = (
            jnp.dot(codes, three, preferred_element_type=F32)
            + jnp.dot(codes, two, preferred_element_type=F32)
            + jnp.dot(codes, one, preferred_element_type=F32)
        )
        first = beta_one * first_ref[...] + (1.0 - beta_one) * proj
        second = beta_two * second_ref[...] + (1.0 - beta_two) * proj * proj
        first_out_ref[...] = first
        second_out_ref[...] = second
        normed = first / first_fix / (jnp.sqrt(second / second_fix) + epsilon)
        high = normed.astype(BF)
        high_ref[...] = high
        low_ref[...] = (normed - high.astype(F32)).astype(BF)

    for n, ref in enumerate((b0, b1, b2, b3)):

        @pl.when(g == n)
        def _(ref=ref):
            rows = ref[pl.ds(pl.multiple_of(j * 768, 256), 768), :]
            out_ref[...] = (dot_nt(low_ref[...], rows) + dot_nt(high_ref[...], rows)).astype(BF)


def update(place, codes, proj, first, second, pieces):
    full = lambda shape: pl.BlockSpec(shape, lambda g, j, s: (0, 0))
    return pl.pallas_call(
        update_kernel,
        grid_spec=pltpu.PrefetchScalarGridSpec(
            num_scalar_prefetch=1,
            grid=(4, 2),
            in_specs=[full((LAT, TOK)), full((TOK, RANK)), full((LAT, RANK)), full((LAT, RANK))]
            + [full((PIECE, RANK))] * 4,
            out_specs=[
                pl.BlockSpec((LAT, 768), lambda g, j, s: (0, (s[4] ^ g) * 2 + j)),
                full((LAT, RANK)),
                full((LAT, RANK)),
            ],
            scratch_shapes=[pltpu.VMEM((LAT, RANK), BF), pltpu.VMEM((LAT, RANK), BF)],
        ),
        out_shape=[
            jax.ShapeDtypeStruct((LAT, MODEL), BF),
            jax.ShapeDtypeStruct((LAT, RANK), F32),
            jax.ShapeDtypeStruct((LAT, RANK), F32),
        ],
        cost_estimate=pl.CostEstimate(
            flops=2 * LAT * RANK * MODEL * 2, bytes_accessed=11_000_000, transcendentals=0
        ),
        name="update",
    )(place, codes, proj, first, second, *pieces)


def shards(codes_val, codes_idx, target, dec_weight, dec_bias, basis, first_mom, second_mom):
    y_x = lax.axis_index(("y", "x_hi"))
    z = lax.axis_index("z")
    block = lax.axis_index(("x_lo", "core"))
    device = (y_x * 8 + z) * 4 + block
    place = jnp.stack([device, y_x, block, z, block]).astype(jnp.int32)
    idx_t = codes_idx.T
    val_t = codes_val.T

    own = basis.astype(BF)
    pairs = []
    for x in range(4):
        pairs.append((((x + 3) % 4) * 2, x * 2))
        pairs.append((((x + 1) % 4) * 2 + 1, x * 2 + 1))
    swap = [(0, 1), (1, 0)]
    other = lax.ppermute(own, RING, pairs)
    own_sib = lax.ppermute(own, "core", swap)
    other_sib = lax.ppermute(other, "core", swap)
    pieces = (own, own_sib, other, other_sib)

    sent, codes = pack(place, idx_t, val_t, dec_weight)
    recv = lax.all_to_all(
        sent.reshape(32, 8, MODEL), PLANE, split_axis=0, concat_axis=0, tiled=True
    ).reshape(TOK, MODEL)
    part, slab = partial_recon(place, idx_t, val_t, recv)
    rows = MODEL // 128
    part = lax.all_to_all(
        part.reshape(8, rows, 128), "z", split_axis=0, concat_axis=0, tiled=True
    )
    recon = jnp.sum(part, axis=0)
    resid = (
        recon + dec_bias.reshape(rows, 128) - target.reshape(rows, 128).astype(F32)
    ).astype(BF)
    resid = lax.all_to_all(
        jnp.broadcast_to(resid[None], (8, rows, 128)), "z", split_axis=0, concat_axis=0, tiled=True
    ).reshape(8, MODEL)
    grad, proj = back(place, resid, recv, slab, pieces)
    proj = lax.all_to_all(proj, PLANE, split_axis=0, concat_axis=0, tiled=True)
    grad = lax.all_to_all(
        grad.reshape(8, 1, 128), "z", split_axis=0, concat_axis=0, tiled=True
    )
    code_grad = jnp.sum(grad, axis=0)[:, :TOPK]
    new, first_out, second_out = update(
        place, codes, proj.reshape(TOK, RANK), first_mom, second_mom, pieces
    )
    return (new, first_out, second_out, code_grad)


def solution(mesh):
    torus = Mesh(mesh.devices.reshape(4, 2, 8, 2, 2), AXES)
    rows = P(AXES, None)
    in_specs = (P(), P(), rows, rows, P(), P(("x_lo", "core"), None), rows, rows)
    return jax.shard_map(
        shards, mesh=torus, in_specs=in_specs, out_specs=(rows, rows, rows, rows), check_vma=False
    )
```

```python
import math

import jax
import jax.numpy as jnp
from jax import lax
from jax.experimental import pallas as pl
from jax.experimental.pallas import tpu as pltpu
from jax.sharding import Mesh
from jax.sharding import PartitionSpec as P


AXES = ("y", "x_hi", "z", "x_lo", "core")
PLANE = ("y", "x_hi", "x_lo", "core")
RING = ("x_hi", "x_lo", "core")

beta_one = 0.9
beta_two = 0.999
epsilon = 1e-08
first_fix = 1.0 - math.exp(100.0 * math.log(0.9))
second_fix = 1.0 - math.exp(100.0 * math.log(0.999))

LAT = 384
TOK = 256
TOPK = 64
MODEL = 6144
RANK = 256
PIECE = MODEL // 4
BF = jnp.bfloat16
F32 = jnp.float32


def iota(shape, dim):
    return lax.broadcasted_iota(jnp.int32, shape, dim)


def dot_nt(a, b):
    return lax.dot_general(a, b, (((1,), (1,)), ((), ())), preferred_element_type=F32)


def slab_of(idx):
    return jnp.floor((idx.astype(F32) + 0.5) * (1.0 / LAT))


def where_am_i():
    y_x = lax.axis_index("y") * 2 + lax.axis_index("x_hi")
    z = lax.axis_index("z")
    block = lax.axis_index("x_lo") * 2 + lax.axis_index("core")
    return y_x, z, block


def pack_kernel(idx_ref, val_ref, weight_ref, sent_ref, codes_ref, hot_ref):
    @pl.when(pl.program_id(0) == 0)
    def _():
        y_x, z, block = where_am_i()
        me = (y_x * 8 + z) * 4 + block
        idx = idx_ref[...]
        inside = slab_of(idx) == me.astype(F32)
        local = jnp.sum(jnp.where(inside, idx - me * LAT + 1, 0), axis=0, keepdims=True) - 1
        value = jnp.sum(
            jnp.where(inside, val_ref[...].astype(F32), 0.0), axis=0, keepdims=True
        )
        hit = iota((LAT, TOK), 0) == local
        row = iota((TOK, TOK), 0)
        token = (row >> 5) * 32 + (row & 7) * 4 + ((row >> 3) & 3)
        order = jnp.where(iota((TOK, TOK), 1) == token, 1.0, 0.0).astype(BF)
        hot_ref[...] = dot_nt(order, jnp.where(hit, 1.0, 0.0).astype(BF)).astype(BF)
        codes_ref[...] = dot_nt(jnp.where(hit, value, 0.0).astype(BF), order).astype(BF)

    sent_ref[...] = jnp.dot(
        hot_ref[...], weight_ref[...], preferred_element_type=F32
    ).astype(BF)


def pack(idx_t, val_t, weight):
    step = 768
    return pl.pallas_call(
        pack_kernel,
        grid=(MODEL // step,),
        in_specs=[
            pl.BlockSpec((TOPK, TOK), lambda j: (0, 0)),
            pl.BlockSpec((TOPK, TOK), lambda j: (0, 0)),
            pl.BlockSpec((LAT, step), lambda j: (0, j)),
        ],
        out_specs=[
            pl.BlockSpec((TOK, step), lambda j: (0, j)),
            pl.BlockSpec((LAT, TOK), lambda j: (0, 0)),
        ],
        scratch_shapes=[pltpu.VMEM((TOK, LAT), BF)],
        out_shape=[
            jax.ShapeDtypeStruct((TOK, MODEL), BF),
            jax.ShapeDtypeStruct((LAT, TOK), BF),
        ],
        cost_estimate=pl.CostEstimate(
            flops=2 * TOK * LAT * MODEL, bytes_accessed=8_000_000, transcendentals=0
        ),
        name="pack",
    )(idx_t, val_t, weight)


def recon_kernel(idx_ref, val_ref, recv_ref, part_ref, slab_ref):
    y_x, z, block = where_am_i()
    token = y_x * 32 + iota((8, TOK), 0) * 4 + block
    pick = jnp.where(iota((8, TOK), 1) == token, 1.0, 0.0).astype(BF)
    slab = dot_nt(pick, slab_of(idx_ref[...]).astype(BF))
    value = dot_nt(pick, val_ref[...])
    slab_ref[...] = slab
    lane = iota((8, TOK), 1)
    source = ((lane >> 5) * 32 + ((lane >> 3) & 3) + z * 4).astype(F32)
    weight = jnp.zeros((8, TOK), F32)
    for k in range(TOPK):
        weight += jnp.where(slab[:, k : k + 1] == source, value[:, k : k + 1], 0.0)
    weight = jnp.where((lane & 7) == iota((8, TOK), 0), weight, 0.0).astype(BF)
    step = 1024
    for j in range(MODEL // step):
        part = jnp.dot(
            weight, recv_ref[:, j * step : (j + 1) * step], preferred_element_type=F32
        )
        for c in range(step // 128):
            part_ref[:, j * (step // 128) + c, :] = part[:, c * 128 : (c + 1) * 128]


def whole(n):
    return [pl.BlockSpec(memory_space=pltpu.VMEM)] * n


def partial_recon(idx_t, val_t, recv):
    return pl.pallas_call(
        recon_kernel,
        in_specs=whole(3),
        out_specs=whole(2),
        out_shape=[
            jax.ShapeDtypeStruct((8, MODEL // 128, 128), F32),
            jax.ShapeDtypeStruct((8, TOPK), F32),
        ],
        cost_estimate=pl.CostEstimate(
            flops=2 * TOK * 8 * MODEL, bytes_accessed=4_000_000, transcendentals=0
        ),
        compiler_params=pltpu.CompilerParams(vmem_limit_bytes=10 * 1024 * 1024),
        name="partial_recon",
    )(idx_t, val_t, recv)


def project_kernel(resid_ref, b0, b1, b2, b3, proj_ref):
    _, _, block = where_am_i()
    proj = jnp.zeros((8, RANK), F32)
    for g, ref in enumerate((b0, b1, b2, b3)):
        at = pl.multiple_of((block ^ g) * PIECE, 128)
        proj += jnp.dot(resid_ref[:, pl.ds(at, PIECE)], ref[...], preferred_element_type=F32)
    proj_ref[...] = jnp.broadcast_to(proj[None], (32, 8, RANK))


def project(resid, pieces):
    return pl.pallas_call(
        project_kernel,
        in_specs=whole(5),
        out_specs=whole(1)[0],
        out_shape=jax.ShapeDtypeStruct((32, 8, RANK), F32),
        cost_estimate=pl.CostEstimate(
            flops=2 * RANK * 8 * MODEL, bytes_accessed=3_500_000, transcendentals=0
        ),
        name="project",
    )(resid, *pieces)


def back_kernel(resid_ref, recv_ref, slab_ref, cg_ref):
    _, z, _ = where_am_i()
    dots = dot_nt(resid_ref[...], recv_ref[...])
    lane = iota((8, TOK), 1)
    dots = jnp.where((lane & 7) == iota((8, TOK), 0), dots, 0.0)
    member = jnp.where(iota((TOK, 128), 0) >> 3 == iota((TOK, 128), 1), 1.0, 0.0)
    dots = jnp.dot(
        dots, member, precision=lax.Precision.HIGHEST, preferred_element_type=F32
    )
    slab = slab_ref[...]
    grad = jnp.zeros((8, TOPK), F32)
    for p in range(32):
        source = ((p >> 2) * 32 + (p & 3) + z * 4).astype(F32)
        grad += jnp.where(slab == source, dots[:, p : p + 1], 0.0)
    cg_ref[:, 0:TOPK] = grad
    cg_ref[:, TOPK:] = jnp.zeros((8, 128 - TOPK), F32)


def back(resid, recv, slab):
    return pl.pallas_call(
        back_kernel,
        in_specs=whole(3),
        out_specs=whole(1)[0],
        out_shape=jax.ShapeDtypeStruct((8, 128), F32),
        cost_estimate=pl.CostEstimate(
            flops=2 * TOK * 8 * MODEL, bytes_accessed=3_500_000, transcendentals=0
        ),
        compiler_params=pltpu.CompilerParams(vmem_limit_bytes=10 * 1024 * 1024),
        name="back",
    )(resid, recv, slab)


def update_kernel(
    place, codes_ref, proj_ref, first_ref, second_ref, b0, b1, b2, b3,
    out_ref, first_out_ref, second_out_ref, high_ref, low_ref,
):
    g = pl.program_id(0)
    j = pl.program_id(1)

    @pl.when((g == 0) & (j == 0))
    def _():
        proj_tok = proj_ref[...]
        codes = codes_ref[...]
        one = proj_tok.astype(BF)
        rest = proj_tok - one.astype(F32)
        two = rest.astype(BF)
        three = (rest - two.astype(F32)).astype(BF)
        proj = (
            jnp.dot(codes, three, preferred_element_type=F32)
            + jnp.dot(codes, two, preferred_element_type=F32)
            + jnp.dot(codes, one, preferred_element_type=F32)
        )
        first = beta_one * first_ref[...] + (1.0 - beta_one) * proj
        second = beta_two * second_ref[...] + (1.0 - beta_two) * proj * proj
        first_out_ref[...] = first
        second_out_ref[...] = second
        normed = first / first_fix / (jnp.sqrt(second / second_fix) + epsilon)
        high = normed.astype(BF)
        high_ref[...] = high
        low_ref[...] = (normed - high.astype(F32)).astype(BF)

    for n, ref in enumerate((b0, b1, b2, b3)):

        @pl.when(g == n)
        def _(ref=ref):
            rows = ref[pl.ds(pl.multiple_of(j * 768, 256), 768), :]
            out_ref[...] = (dot_nt(low_ref[...], rows) + dot_nt(high_ref[...], rows)).astype(BF)


def update(place, codes, proj, first, second, pieces):
    full = lambda shape: pl.BlockSpec(shape, lambda g, j, s: (0, 0))
    return pl.pallas_call(
        update_kernel,
        grid_spec=pltpu.PrefetchScalarGridSpec(
            num_scalar_prefetch=1,
            grid=(4, 2),
            in_specs=[full((LAT, TOK)), full((TOK, RANK)), full((LAT, RANK)), full((LAT, RANK))]
            + [full((PIECE, RANK))] * 4,
            out_specs=[
                pl.BlockSpec((LAT, 768), lambda g, j, s: (0, (s[0] ^ g) * 2 + j)),
                full((LAT, RANK)),
                full((LAT, RANK)),
            ],
            scratch_shapes=[pltpu.VMEM((LAT, RANK), BF), pltpu.VMEM((LAT, RANK), BF)],
        ),
        out_shape=[
            jax.ShapeDtypeStruct((LAT, MODEL), BF),
            jax.ShapeDtypeStruct((LAT, RANK), F32),
            jax.ShapeDtypeStruct((LAT, RANK), F32),
        ],
        cost_estimate=pl.CostEstimate(
            flops=2 * LAT * RANK * MODEL * 2, bytes_accessed=11_000_000, transcendentals=0
        ),
        name="update",
    )(place, codes, proj, first, second, *pieces)


def step(codes_val, codes_idx, target, dec_weight, dec_bias, basis, first_mom, second_mom):
    block = lax.axis_index(("x_lo", "core")).astype(jnp.int32)
    place = block[None]
    idx_t = codes_idx.T
    val_t = codes_val.T
    exchange = lambda a, axes: lax.all_to_all(a, axes, split_axis=0, concat_axis=0, tiled=True)
    swap = [(0, 1), (1, 0)]
    pairs = []
    for x in range(4):
        pairs.append((((x + 3) % 4) * 2, x * 2))
        pairs.append((((x + 1) % 4) * 2 + 1, x * 2 + 1))

    sent, codes = pack(idx_t, val_t, dec_weight)
    recv = exchange(sent.reshape(32, 8, MODEL), PLANE).reshape(TOK, MODEL)
    own = basis.astype(BF)
    own_sib = lax.ppermute(own, "core", swap)
    part, slab = partial_recon(idx_t, val_t, recv)
    late, recv = lax.optimization_barrier((own, recv))
    other = lax.ppermute(late, RING, pairs)
    other_sib = lax.ppermute(other, "core", swap)
    pieces = (own, own_sib, other, other_sib)
    rows = MODEL // 128
    part = exchange(part, "z")
    recon = jnp.sum(part, axis=0)
    resid = (recon + dec_bias.reshape(rows, 128) - target.reshape(rows, 128).astype(F32)).astype(BF)
    resid = exchange(jnp.broadcast_to(resid[None], (8, rows, 128)), "z").reshape(8, MODEL)
    proj = project(resid, pieces)
    proj = exchange(proj, PLANE)
    grad = back(resid, recv, slab)
    grad = exchange(grad.reshape(8, 1, 128), "z")
    code_grad = jnp.sum(grad, axis=0)[:, :TOPK]
    new, first_out, second_out = update(
        place, codes, proj.reshape(TOK, RANK), first_mom, second_mom, pieces
    )
    return (new, first_out, second_out, code_grad)


def solution(mesh):
    torus = Mesh(mesh.devices.reshape(4, 2, 8, 2, 2), AXES)
    rows = P(AXES, None)
    in_specs = (P(), P(), rows, rows, P(), P(("x_lo", "core"), None), rows, rows)
    return jax.shard_map(
        step, mesh=torus, in_specs=in_specs, out_specs=(rows, rows, rows, rows), check_vma=False
    )
```

```python
import math

import jax
import jax.numpy as jnp
from jax import lax
from jax.experimental import pallas as pl
from jax.experimental.pallas import tpu as pltpu
from jax.sharding import Mesh
from jax.sharding import PartitionSpec as P


AXES = ("y", "x_hi", "z", "x_lo", "core")
PLANE = ("y", "x_hi", "x_lo", "core")
RING = ("x_hi", "x_lo", "core")

beta_one = 0.9
beta_two = 0.999
epsilon = 1e-08
first_fix = 1.0 - math.exp(100.0 * math.log(0.9))
second_fix = 1.0 - math.exp(100.0 * math.log(0.999))

LAT = 384
TOK = 256
TOPK = 64
MODEL = 6144
RANK = 256
PIECE = MODEL // 4
PACK = 4
BF = jnp.bfloat16
F32 = jnp.float32


def iota(shape, dim):
    return lax.broadcasted_iota(jnp.int32, shape, dim)


def dot_nt(a, b):
    return lax.dot_general(a, b, (((1,), (1,)), ((), ())), preferred_element_type=F32)


def slab_of(idx):
    return jnp.floor((idx.astype(F32) + 0.5) * (1.0 / LAT))


def whole(n):
    return [pl.BlockSpec(memory_space=pltpu.VMEM)] * n


def where_am_i():
    y_x = lax.axis_index("y") * 2 + lax.axis_index("x_hi")
    z = lax.axis_index("z")
    block = lax.axis_index("x_lo") * 2 + lax.axis_index("core")
    return y_x, z, block


def pack_kernel(
    idx_hbm, val_hbm, weight_ref, sent_ref, codes_hbm,
    idx_ref, val_ref, codes_ref, in_ref, out_ref, in_sem, out_sem, sem,
):
    width = MODEL // PACK
    cuts = [pl.ds(c * width, width) for c in range(PACK)]
    loads = [
        pltpu.make_async_copy(weight_ref.at[:, cut], in_ref.at[:, cut], in_sem.at[c])
        for c, cut in enumerate(cuts)
    ]
    stores = [
        pltpu.make_async_copy(out_ref.at[:, cut], sent_ref.at[:, cut], out_sem.at[c])
        for c, cut in enumerate(cuts)
    ]
    tables = [
        pltpu.make_async_copy(idx_hbm, idx_ref, sem.at[0]),
        pltpu.make_async_copy(val_hbm, val_ref, sem.at[1]),
    ]
    for load in tables + loads:
        load.start()
    for load in tables:
        load.wait()
    y_x, z, block = where_am_i()
    me = (y_x * 8 + z) * 4 + block
    idx = idx_ref[...]
    inside = slab_of(idx) == me.astype(F32)
    local = jnp.sum(jnp.where(inside, idx - me * LAT + 1, 0), axis=0, keepdims=True) - 1
    value = jnp.sum(jnp.where(inside, val_ref[...].astype(F32), 0.0), axis=0, keepdims=True)
    hit = iota((LAT, TOK), 0) == local
    row = iota((TOK, TOK), 0)
    token = (row >> 5) * 32 + (row & 7) * 4 + ((row >> 3) & 3)
    order = jnp.where(iota((TOK, TOK), 1) == token, 1.0, 0.0).astype(BF)
    hot = dot_nt(order, jnp.where(hit, 1.0, 0.0).astype(BF)).astype(BF)
    for c, cut in enumerate(cuts):
        loads[c].wait()
        out_ref[:, cut] = jnp.dot(
            hot, in_ref[:, cut], preferred_element_type=F32
        ).astype(BF)
        stores[c].start()
    codes_ref[...] = dot_nt(jnp.where(hit, value, 0.0).astype(BF), order).astype(BF)
    store = pltpu.make_async_copy(codes_ref, codes_hbm, sem.at[2])
    store.start()
    for store in stores + [store]:
        store.wait()


ANY = pl.BlockSpec(memory_space=pl.ANY)


def pack(idx_t, val_t, weight):
    return pl.pallas_call(
        pack_kernel,
        in_specs=[ANY] * 3,
        out_specs=[ANY] * 2,
        out_shape=[
            jax.ShapeDtypeStruct((TOK, MODEL), BF),
            jax.ShapeDtypeStruct((LAT, TOK), BF),
        ],
        scratch_shapes=[
            pltpu.VMEM((TOPK, TOK), jnp.int32),
            pltpu.VMEM((TOPK, TOK), BF),
            pltpu.VMEM((LAT, TOK), BF),
            pltpu.VMEM((LAT, MODEL), BF),
            pltpu.VMEM((TOK, MODEL), BF),
            pltpu.SemaphoreType.DMA((PACK,)),
            pltpu.SemaphoreType.DMA((PACK,)),
            pltpu.SemaphoreType.DMA((3,)),
        ],
        cost_estimate=pl.CostEstimate(
            flops=2 * TOK * LAT * MODEL, bytes_accessed=8_000_000, transcendentals=0
        ),
        name="pack",
    )(idx_t, val_t, weight)


def recon_kernel(idx_ref, val_ref, recv_ref, part_ref, slab_ref):
    y_x, z, block = where_am_i()
    token = y_x * 32 + iota((8, TOK), 0) * 4 + block
    pick = jnp.where(iota((8, TOK), 1) == token, 1.0, 0.0).astype(BF)
    slab = dot_nt(pick, slab_of(idx_ref[...]).astype(BF))
    value = dot_nt(pick, val_ref[...])
    slab_ref[...] = slab
    lane = iota((8, TOK), 1)
    source = ((lane >> 5) * 32 + ((lane >> 3) & 3) + z * 4).astype(F32)
    weight = jnp.zeros((8, TOK), F32)
    for k in range(TOPK):
        weight += jnp.where(slab[:, k : k + 1] == source, value[:, k : k + 1], 0.0)
    weight = jnp.where((lane & 7) == iota((8, TOK), 0), weight, 0.0).astype(BF)
    step = 1024
    for j in range(MODEL // step):
        part = jnp.dot(
            weight, recv_ref[:, j * step : (j + 1) * step], preferred_element_type=F32
        )
        for c in range(step // 128):
            part_ref[:, j * (step // 128) + c, :] = part[:, c * 128 : (c + 1) * 128]


def partial_recon(idx_t, val_t, recv):
    return pl.pallas_call(
        recon_kernel,
        in_specs=whole(3),
        out_specs=whole(2),
        out_shape=[
            jax.ShapeDtypeStruct((8, MODEL // 128, 128), F32),
            jax.ShapeDtypeStruct((8, TOPK), F32),
        ],
        cost_estimate=pl.CostEstimate(
            flops=2 * TOK * 8 * MODEL, bytes_accessed=4_000_000, transcendentals=0
        ),
        compiler_params=pltpu.CompilerParams(vmem_limit_bytes=10 * 1024 * 1024),
        name="partial_recon",
    )(idx_t, val_t, recv)


def resid_kernel(part_ref, bias_ref, target_ref, resid_ref):
    recon = jnp.sum(part_ref[...], axis=0)
    resid = recon + bias_ref[...] - target_ref[...].astype(F32)
    resid_ref[...] = jnp.broadcast_to(resid.astype(BF)[None], resid_ref.shape)


def residual(part, bias, target):
    return pl.pallas_call(
        resid_kernel,
        in_specs=whole(3),
        out_specs=whole(1)[0],
        out_shape=jax.ShapeDtypeStruct((8, MODEL // 128, 128), BF),
        cost_estimate=pl.CostEstimate(
            flops=10 * MODEL, bytes_accessed=400_000, transcendentals=0
        ),
        compiler_params=pltpu.CompilerParams(vmem_limit_bytes=10 * 1024 * 1024),
        name="residual",
    )(part, bias, target)


def load_pieces(sources, buf_ref, sem):
    loads = [
        pltpu.make_async_copy(source, buf_ref.at[n], sem.at[n])
        for n, source in enumerate(sources)
    ]
    for load in loads:
        load.start()
    return loads


PIECES = [pltpu.VMEM((4, PIECE, RANK), BF), pltpu.SemaphoreType.DMA((4,))]


def project_kernel(resid_ref, b0, b1, b2, b3, proj_ref):
    _, _, block = where_am_i()
    proj = jnp.zeros((8, RANK), F32)
    for n, ref in enumerate((b0, b1, b2, b3)):
        at = pl.multiple_of((block ^ n) * PIECE, 128)
        proj += jnp.dot(resid_ref[:, pl.ds(at, PIECE)], ref[...], preferred_element_type=F32)
    proj_ref[...] = jnp.broadcast_to(proj[None], (32, 8, RANK))


def project(resid, pieces):
    return pl.pallas_call(
        project_kernel,
        in_specs=whole(5),
        out_specs=whole(1)[0],
        out_shape=jax.ShapeDtypeStruct((32, 8, RANK), F32),
        cost_estimate=pl.CostEstimate(
            flops=2 * RANK * 8 * MODEL, bytes_accessed=3_500_000, transcendentals=0
        ),
        name="project",
    )(resid, *pieces)


def back_kernel(resid_ref, recv_ref, slab_ref, cg_ref):
    _, z, _ = where_am_i()
    dots = dot_nt(resid_ref[...], recv_ref[...])
    lane = iota((8, TOK), 1)
    dots = jnp.where((lane & 7) == iota((8, TOK), 0), dots, 0.0)
    member = jnp.where(iota((TOK, 128), 0) >> 3 == iota((TOK, 128), 1), 1.0, 0.0)
    dots = jnp.dot(
        dots, member, precision=lax.Precision.HIGHEST, preferred_element_type=F32
    )
    slab = slab_ref[...]
    grad = jnp.zeros((8, TOPK), F32)
    for p in range(32):
        source = ((p >> 2) * 32 + (p & 3) + z * 4).astype(F32)
        grad += jnp.where(slab == source, dots[:, p : p + 1], 0.0)
    cg_ref[:, 0:TOPK] = grad
    cg_ref[:, TOPK:] = jnp.zeros((8, 128 - TOPK), F32)


def back(resid, recv, slab):
    return pl.pallas_call(
        back_kernel,
        in_specs=whole(3),
        out_specs=whole(1)[0],
        out_shape=jax.ShapeDtypeStruct((8, 128), F32),
        cost_estimate=pl.CostEstimate(
            flops=2 * TOK * 8 * MODEL, bytes_accessed=3_500_000, transcendentals=0
        ),
        compiler_params=pltpu.CompilerParams(vmem_limit_bytes=10 * 1024 * 1024),
        name="back",
    )(resid, recv, slab)


def update_kernel(
    codes_hbm, proj_hbm, first_ref, second_ref, b0, b1, b2, b3,
    new_ref, first_out_ref, second_out_ref,
    codes_ref, proj_ref, out_ref, mom_in_ref, mom_out_ref, sem, mom_sem, buf_ref, buf_sem,
):
    _, _, block = where_am_i()
    tables = [
        pltpu.make_async_copy(proj_hbm, proj_ref, mom_sem.at[4]),
        pltpu.make_async_copy(codes_hbm, codes_ref, mom_sem.at[5]),
    ]
    moments = [
        pltpu.make_async_copy(first_ref, mom_in_ref.at[0], mom_sem.at[0]),
        pltpu.make_async_copy(second_ref, mom_in_ref.at[1], mom_sem.at[1]),
    ]
    for load in tables + moments:
        load.start()
    loads = load_pieces((b0, b1, b2, b3), buf_ref, buf_sem)
    for load in tables:
        load.wait()
    proj_tok = proj_ref[...]
    codes = codes_ref[...]
    one = proj_tok.astype(BF)
    rest = proj_tok - one.astype(F32)
    two = rest.astype(BF)
    three = (rest - two.astype(F32)).astype(BF)
    proj = (
        jnp.dot(codes, three, preferred_element_type=F32)
        + jnp.dot(codes, two, preferred_element_type=F32)
        + jnp.dot(codes, one, preferred_element_type=F32)
    )
    for load in moments:
        load.wait()
    first = beta_one * mom_in_ref[0] + (1.0 - beta_one) * proj
    second = beta_two * mom_in_ref[1] + (1.0 - beta_two) * proj * proj
    mom_out_ref[0] = first
    mom_out_ref[1] = second
    stores = [
        pltpu.make_async_copy(mom_out_ref.at[0], first_out_ref, mom_sem.at[2]),
        pltpu.make_async_copy(mom_out_ref.at[1], second_out_ref, mom_sem.at[3]),
    ]
    for store in stores:
        store.start()
    normed = first / first_fix / (jnp.sqrt(second / second_fix) + epsilon)
    high = normed.astype(BF)
    low = (normed - high.astype(F32)).astype(BF)
    width = PIECE // 2
    for n in range(4):
        loads[n].wait()
        for j in range(2):
            rows = buf_ref[n, j * width : (j + 1) * width, :]
            cut = pl.ds((2 * n + j) * width, width)
            out_ref[:, cut] = (dot_nt(low, rows) + dot_nt(high, rows)).astype(BF)
            at = pl.multiple_of((block ^ n) * PIECE + j * width, 128)
            store = pltpu.make_async_copy(
                out_ref.at[:, cut], new_ref.at[:, pl.ds(at, width)], sem.at[2 * n + j]
            )
            store.start()
            stores.append(store)
    for store in stores:
        store.wait()


def update(codes, proj, first, second, pieces):
    return pl.pallas_call(
        update_kernel,
        in_specs=[ANY] * 8,
        out_specs=[ANY] * 3,
        out_shape=[
            jax.ShapeDtypeStruct((LAT, MODEL), BF),
            jax.ShapeDtypeStruct((LAT, RANK), F32),
            jax.ShapeDtypeStruct((LAT, RANK), F32),
        ],
        scratch_shapes=[
            pltpu.VMEM((LAT, TOK), BF),
            pltpu.VMEM((TOK, RANK), F32),
            pltpu.VMEM((LAT, MODEL), BF),
            pltpu.VMEM((2, LAT, RANK), F32),
            pltpu.VMEM((2, LAT, RANK), F32),
            pltpu.SemaphoreType.DMA((8,)),
            pltpu.SemaphoreType.DMA((6,)),
        ]
        + PIECES,
        cost_estimate=pl.CostEstimate(
            flops=2 * LAT * RANK * MODEL * 2, bytes_accessed=11_000_000, transcendentals=0
        ),
        name="update",
    )(codes, proj, first, second, *pieces)


def step(codes_val, codes_idx, target, dec_weight, dec_bias, basis, first_mom, second_mom):
    idx_t = codes_idx.T
    val_t = codes_val.T
    exchange = lambda a, axes: lax.all_to_all(a, axes, split_axis=0, concat_axis=0, tiled=True)
    swap = [(0, 1), (1, 0)]
    straight = []
    crossed = []
    for x in range(4):
        left = ((x + 3) % 4) * 2
        right = ((x + 1) % 4) * 2 + 1
        straight += [(left, x * 2), (right, x * 2 + 1)]
        crossed += [(right - 1, x * 2 + 1), (left + 1, x * 2)]

    rows = MODEL // 128
    sent, codes = pack(idx_t, val_t, dec_weight)
    recv = exchange(sent.reshape(32, 8, MODEL), PLANE).reshape(TOK, MODEL)
    own = basis.astype(BF)
    own_sib = lax.ppermute(own, "core", swap)
    part, slab = partial_recon(idx_t, val_t, recv)
    target = target.reshape(rows, 128)
    late, recv, target = lax.optimization_barrier((own, recv, target))
    other = lax.ppermute(late, RING, straight)
    other_sib = lax.ppermute(late, RING, crossed)
    pieces = (own, own_sib, other, other_sib)
    part = exchange(part, "z")
    resid = residual(part, dec_bias.reshape(rows, 128), target)
    resid = exchange(resid, "z").reshape(8, MODEL)
    proj = project(resid, pieces)
    proj = exchange(proj, PLANE)
    grad = back(resid, recv, slab)
    grad = exchange(grad.reshape(8, 1, 128), "z")
    code_grad = jnp.sum(grad, axis=0)[:, :TOPK]
    new, first_out, second_out = update(
        codes, proj.reshape(TOK, RANK), first_mom, second_mom, pieces
    )
    return (new, first_out, second_out, code_grad)


def solution(mesh):
    torus = Mesh(mesh.devices.reshape(4, 2, 8, 2, 2), AXES)
    rows = P(AXES, None)
    in_specs = (P(), P(), rows, rows, P(), P(("x_lo", "core"), None), rows, rows)
    return jax.shard_map(
        step, mesh=torus, in_specs=in_specs, out_specs=(rows, rows, rows, rows), check_vma=False
    )
```

```python
import math

import jax
import jax.numpy as jnp
from jax import lax
from jax.experimental import pallas as pl
from jax.experimental.pallas import tpu as pltpu
from jax.sharding import Mesh
from jax.sharding import PartitionSpec as P


AXES = ("y", "x_hi", "z", "x_lo", "core")
PLANE = ("y", "x_hi", "x_lo", "core")
RING = ("x_hi", "x_lo", "core")

beta_one = 0.9
beta_two = 0.999
epsilon = 1e-08
first_fix = 1.0 - math.exp(100.0 * math.log(0.9))
second_fix = 1.0 - math.exp(100.0 * math.log(0.999))

LAT = 384
TOK = 256
TOPK = 64
MODEL = 6144
RANK = 256
PIECE = MODEL // 4
PACK = 4
BF = jnp.bfloat16
F32 = jnp.float32


def iota(shape, dim):
    return lax.broadcasted_iota(jnp.int32, shape, dim)


def dot_nt(a, b):
    return lax.dot_general(a, b, (((1,), (1,)), ((), ())), preferred_element_type=F32)


def slab_of(idx):
    return jnp.floor((idx.astype(F32) + 0.5) * (1.0 / LAT))


def whole(n):
    return [pl.BlockSpec(memory_space=pltpu.VMEM)] * n


def where_am_i():
    y_x = lax.axis_index("y") * 2 + lax.axis_index("x_hi")
    z = lax.axis_index("z")
    block = lax.axis_index("x_lo") * 2 + lax.axis_index("core")
    return y_x, z, block


def pack_kernel(
    idx_hbm, val_hbm, weight_ref, sent_ref, codes_hbm,
    idx_ref, val_ref, codes_ref, in_ref, out_ref, in_sem, out_sem, sem,
):
    width = MODEL // PACK
    cuts = [pl.ds(c * width, width) for c in range(PACK)]
    loads = [
        pltpu.make_async_copy(weight_ref.at[:, cut], in_ref.at[:, cut], in_sem.at[c])
        for c, cut in enumerate(cuts)
    ]
    stores = [
        pltpu.make_async_copy(out_ref.at[:, cut], sent_ref.at[:, cut], out_sem.at[c])
        for c, cut in enumerate(cuts)
    ]
    tables = [
        pltpu.make_async_copy(idx_hbm, idx_ref, sem.at[0]),
        pltpu.make_async_copy(val_hbm, val_ref, sem.at[1]),
    ]
    for load in tables + loads:
        load.start()
    for load in tables:
        load.wait()
    y_x, z, block = where_am_i()
    me = (y_x * 8 + z) * 4 + block
    idx = idx_ref[...]
    inside = slab_of(idx) == me.astype(F32)
    local = jnp.sum(jnp.where(inside, idx - me * LAT + 1, 0), axis=0, keepdims=True) - 1
    value = jnp.sum(jnp.where(inside, val_ref[...].astype(F32), 0.0), axis=0, keepdims=True)
    hit = iota((LAT, TOK), 0) == local
    row = iota((TOK, TOK), 0)
    token = (row >> 5) * 32 + (row & 7) * 4 + ((row >> 3) & 3)
    order = jnp.where(iota((TOK, TOK), 1) == token, 1.0, 0.0).astype(BF)
    hot = dot_nt(order, jnp.where(hit, 1.0, 0.0).astype(BF)).astype(BF)
    for c, cut in enumerate(cuts):
        loads[c].wait()
        out_ref[:, cut] = jnp.dot(
            hot, in_ref[:, cut], preferred_element_type=F32
        ).astype(BF)
        stores[c].start()
    codes_ref[...] = dot_nt(jnp.where(hit, value, 0.0).astype(BF), order).astype(BF)
    store = pltpu.make_async_copy(codes_ref, codes_hbm, sem.at[2])
    store.start()
    for store in stores + [store]:
        store.wait()


ANY = pl.BlockSpec(memory_space=pl.ANY)


def pack(idx_t, val_t, weight):
    return pl.pallas_call(
        pack_kernel,
        in_specs=[ANY] * 3,
        out_specs=[ANY] * 2,
        out_shape=[
            jax.ShapeDtypeStruct((TOK, MODEL), BF),
            jax.ShapeDtypeStruct((LAT, TOK), BF),
        ],
        scratch_shapes=[
            pltpu.VMEM((TOPK, TOK), jnp.int32),
            pltpu.VMEM((TOPK, TOK), BF),
            pltpu.VMEM((LAT, TOK), BF),
            pltpu.VMEM((LAT, MODEL), BF),
            pltpu.VMEM((TOK, MODEL), BF),
            pltpu.SemaphoreType.DMA((PACK,)),
            pltpu.SemaphoreType.DMA((PACK,)),
            pltpu.SemaphoreType.DMA((3,)),
        ],
        cost_estimate=pl.CostEstimate(
            flops=2 * TOK * LAT * MODEL, bytes_accessed=8_000_000, transcendentals=0
        ),
        name="pack",
    )(idx_t, val_t, weight)


def select_kernel(idx_ref, val_ref, weight_ref, slab_ref):
    y_x, z, block = where_am_i()
    token = y_x * 32 + iota((8, TOK), 0) * 4 + block
    pick = jnp.where(iota((8, TOK), 1) == token, 1.0, 0.0).astype(BF)
    slab = dot_nt(pick, slab_of(idx_ref[...]).astype(BF))
    value = dot_nt(pick, val_ref[...])
    slab_ref[...] = slab
    lane = iota((8, TOK), 1)
    source = ((lane >> 5) * 32 + ((lane >> 3) & 3) + z * 4).astype(F32)
    weight = jnp.zeros((8, TOK), F32)
    for k in range(TOPK):
        weight += jnp.where(slab[:, k : k + 1] == source, value[:, k : k + 1], 0.0)
    weight_ref[...] = jnp.where((lane & 7) == iota((8, TOK), 0), weight, 0.0).astype(BF)


def select(idx_t, val_t):
    return pl.pallas_call(
        select_kernel,
        in_specs=whole(2),
        out_specs=whole(2),
        out_shape=[
            jax.ShapeDtypeStruct((8, TOK), BF),
            jax.ShapeDtypeStruct((8, TOPK), F32),
        ],
        cost_estimate=pl.CostEstimate(
            flops=20_000_000, bytes_accessed=200_000, transcendentals=0
        ),
        compiler_params=pltpu.CompilerParams(vmem_limit_bytes=10 * 1024 * 1024),
        name="select",
    )(idx_t, val_t)


def recon_kernel(weight_ref, recv_ref, part_ref):
    weight = weight_ref[...]
    step = 1024
    for j in range(MODEL // step):
        part = jnp.dot(
            weight, recv_ref[:, j * step : (j + 1) * step], preferred_element_type=F32
        )
        for c in range(step // 128):
            part_ref[:, j * (step // 128) + c, :] = part[:, c * 128 : (c + 1) * 128]


def partial_recon(weight, recv):
    return pl.pallas_call(
        recon_kernel,
        in_specs=whole(2),
        out_specs=whole(1)[0],
        out_shape=jax.ShapeDtypeStruct((8, MODEL // 128, 128), F32),
        cost_estimate=pl.CostEstimate(
            flops=2 * TOK * 8 * MODEL, bytes_accessed=4_000_000, transcendentals=0
        ),
        compiler_params=pltpu.CompilerParams(vmem_limit_bytes=10 * 1024 * 1024),
        name="partial_recon",
    )(weight, recv)


def resid_kernel(part_ref, bias_ref, target_ref, resid_ref):
    recon = jnp.sum(part_ref[...], axis=0)
    resid = recon + bias_ref[...] - target_ref[...].astype(F32)
    resid_ref[...] = jnp.broadcast_to(resid.astype(BF)[None], resid_ref.shape)


def residual(part, bias, target):
    return pl.pallas_call(
        resid_kernel,
        in_specs=whole(3),
        out_specs=whole(1)[0],
        out_shape=jax.ShapeDtypeStruct((8, MODEL // 128, 128), BF),
        cost_estimate=pl.CostEstimate(
            flops=10 * MODEL, bytes_accessed=400_000, transcendentals=0
        ),
        compiler_params=pltpu.CompilerParams(vmem_limit_bytes=10 * 1024 * 1024),
        name="residual",
    )(part, bias, target)


def load_pieces(sources, buf_ref, sem):
    loads = [
        pltpu.make_async_copy(source, buf_ref.at[n], sem.at[n])
        for n, source in enumerate(sources)
    ]
    for load in loads:
        load.start()
    return loads


PIECES = [pltpu.VMEM((4, PIECE, RANK), BF), pltpu.SemaphoreType.DMA((4,))]


def project_kernel(resid_ref, b0, b1, b2, b3, proj_ref):
    _, _, block = where_am_i()
    proj = jnp.zeros((8, RANK), F32)
    for n, ref in enumerate((b0, b1, b2, b3)):
        at = pl.multiple_of((block ^ n) * PIECE, 128)
        proj += jnp.dot(resid_ref[:, pl.ds(at, PIECE)], ref[...], preferred_element_type=F32)
    proj_ref[...] = jnp.broadcast_to(proj[None], (32, 8, RANK))


def project(resid, pieces):
    return pl.pallas_call(
        project_kernel,
        in_specs=whole(5),
        out_specs=whole(1)[0],
        out_shape=jax.ShapeDtypeStruct((32, 8, RANK), F32),
        cost_estimate=pl.CostEstimate(
            flops=2 * RANK * 8 * MODEL, bytes_accessed=3_500_000, transcendentals=0
        ),
        name="project",
    )(resid, *pieces)


def back_kernel(resid_ref, recv_ref, slab_ref, cg_ref):
    _, z, _ = where_am_i()
    dots = dot_nt(resid_ref[...], recv_ref[...])
    lane = iota((8, TOK), 1)
    dots = jnp.where((lane & 7) == iota((8, TOK), 0), dots, 0.0)
    member = jnp.where(iota((TOK, 128), 0) >> 3 == iota((TOK, 128), 1), 1.0, 0.0)
    dots = jnp.dot(
        dots, member, precision=lax.Precision.HIGHEST, preferred_element_type=F32
    )
    slab = slab_ref[...]
    grad = jnp.zeros((8, TOPK), F32)
    for p in range(32):
        source = ((p >> 2) * 32 + (p & 3) + z * 4).astype(F32)
        grad += jnp.where(slab == source, dots[:, p : p + 1], 0.0)
    cg_ref[:, 0:TOPK] = grad
    cg_ref[:, TOPK:] = jnp.zeros((8, 128 - TOPK), F32)


def back(resid, recv, slab):
    return pl.pallas_call(
        back_kernel,
        in_specs=whole(3),
        out_specs=whole(1)[0],
        out_shape=jax.ShapeDtypeStruct((8, 128), F32),
        cost_estimate=pl.CostEstimate(
            flops=2 * TOK * 8 * MODEL, bytes_accessed=3_500_000, transcendentals=0
        ),
        compiler_params=pltpu.CompilerParams(vmem_limit_bytes=10 * 1024 * 1024),
        name="back",
    )(resid, recv, slab)


def update_kernel(
    codes_hbm, proj_hbm, first_ref, second_ref, b0, b1, b2, b3,
    new_ref, first_out_ref, second_out_ref,
    codes_ref, proj_ref, out_ref, mom_in_ref, mom_out_ref, sem, mom_sem, buf_ref, buf_sem,
):
    _, _, block = where_am_i()
    tables = [
        pltpu.make_async_copy(proj_hbm, proj_ref, mom_sem.at[4]),
        pltpu.make_async_copy(codes_hbm, codes_ref, mom_sem.at[5]),
    ]
    moments = [
        pltpu.make_async_copy(first_ref, mom_in_ref.at[0], mom_sem.at[0]),
        pltpu.make_async_copy(second_ref, mom_in_ref.at[1], mom_sem.at[1]),
    ]
    for load in tables + moments:
        load.start()
    loads = load_pieces((b0, b1, b2, b3), buf_ref, buf_sem)
    for load in tables:
        load.wait()
    proj_tok = proj_ref[...]
    codes = codes_ref[...]
    one = proj_tok.astype(BF)
    rest = proj_tok - one.astype(F32)
    two = rest.astype(BF)
    three = (rest - two.astype(F32)).astype(BF)
    proj = (
        jnp.dot(codes, three, preferred_element_type=F32)
        + jnp.dot(codes, two, preferred_element_type=F32)
        + jnp.dot(codes, one, preferred_element_type=F32)
    )
    for load in moments:
        load.wait()
    first = beta_one * mom_in_ref[0] + (1.0 - beta_one) * proj
    second = beta_two * mom_in_ref[1] + (1.0 - beta_two) * proj * proj
    mom_out_ref[0] = first
    mom_out_ref[1] = second
    stores = [
        pltpu.make_async_copy(mom_out_ref.at[0], first_out_ref, mom_sem.at[2]),
        pltpu.make_async_copy(mom_out_ref.at[1], second_out_ref, mom_sem.at[3]),
    ]
    for store in stores:
        store.start()
    normed = first / first_fix / (jnp.sqrt(second / second_fix) + epsilon)
    high = normed.astype(BF)
    low = (normed - high.astype(F32)).astype(BF)
    width = PIECE // 2
    for n in range(4):
        loads[n].wait()
        for j in range(2):
            rows = buf_ref[n, j * width : (j + 1) * width, :]
            cut = pl.ds((2 * n + j) * width, width)
            out_ref[:, cut] = (dot_nt(low, rows) + dot_nt(high, rows)).astype(BF)
            at = pl.multiple_of((block ^ n) * PIECE + j * width, 128)
            store = pltpu.make_async_copy(
                out_ref.at[:, cut], new_ref.at[:, pl.ds(at, width)], sem.at[2 * n + j]
            )
            store.start()
            stores.append(store)
    for store in stores:
        store.wait()


def update(codes, proj, first, second, pieces):
    return pl.pallas_call(
        update_kernel,
        in_specs=[ANY] * 8,
        out_specs=[ANY] * 3,
        out_shape=[
            jax.ShapeDtypeStruct((LAT, MODEL), BF),
            jax.ShapeDtypeStruct((LAT, RANK), F32),
            jax.ShapeDtypeStruct((LAT, RANK), F32),
        ],
        scratch_shapes=[
            pltpu.VMEM((LAT, TOK), BF),
            pltpu.VMEM((TOK, RANK), F32),
            pltpu.VMEM((LAT, MODEL), BF),
            pltpu.VMEM((2, LAT, RANK), F32),
            pltpu.VMEM((2, LAT, RANK), F32),
            pltpu.SemaphoreType.DMA((8,)),
            pltpu.SemaphoreType.DMA((6,)),
        ]
        + PIECES,
        cost_estimate=pl.CostEstimate(
            flops=2 * LAT * RANK * MODEL * 2, bytes_accessed=11_000_000, transcendentals=0
        ),
        name="update",
    )(codes, proj, first, second, *pieces)


def step(codes_val, codes_idx, target, dec_weight, dec_bias, basis, first_mom, second_mom):
    idx_t = codes_idx.T
    val_t = codes_val.T
    exchange = lambda a, axes: lax.all_to_all(a, axes, split_axis=0, concat_axis=0, tiled=True)
    swap = [(0, 1), (1, 0)]
    straight = []
    crossed = []
    for x in range(4):
        left = ((x + 3) % 4) * 2
        right = ((x + 1) % 4) * 2 + 1
        straight += [(left, x * 2), (right, x * 2 + 1)]
        crossed += [(right - 1, x * 2 + 1), (left + 1, x * 2)]

    rows = MODEL // 128
    sent, codes = pack(idx_t, val_t, dec_weight)
    recv = exchange(sent.reshape(32, 8, MODEL), PLANE).reshape(TOK, MODEL)
    own = basis.astype(BF)
    own_sib = lax.ppermute(own, "core", swap)
    weight, slab = select(idx_t, val_t)
    part = partial_recon(weight, recv)
    target = target.reshape(rows, 128)
    late, recv, target = lax.optimization_barrier((own, recv, target))
    other = lax.ppermute(late, RING, straight)
    other_sib = lax.ppermute(late, RING, crossed)
    pieces = (own, own_sib, other, other_sib)
    part = exchange(part, "z")
    resid = residual(part, dec_bias.reshape(rows, 128), target)
    resid = exchange(resid, "z").reshape(8, MODEL)
    proj = project(resid, pieces)
    proj = exchange(proj, PLANE)
    grad = back(resid, recv, slab)
    grad = exchange(grad.reshape(8, 1, 128), "z")
    code_grad = jnp.sum(grad, axis=0)[:, :TOPK]
    new, first_out, second_out = update(
        codes, proj.reshape(TOK, RANK), first_mom, second_mom, pieces
    )
    return (new, first_out, second_out, code_grad)


def solution(mesh):
    torus = Mesh(mesh.devices.reshape(4, 2, 8, 2, 2), AXES)
    rows = P(AXES, None)
    in_specs = (P(), P(), rows, rows, P(), P(("x_lo", "core"), None), rows, rows)
    return jax.shard_map(
        step, mesh=torus, in_specs=in_specs, out_specs=(rows, rows, rows, rows), check_vma=False
    )
```
